768 devices in a mesh: dp: 64 (over x, y, core), fsdp: 12 (over z).
Axes of the slice: x: 4, y: 8, z: 12, core: 2. Of those that a mesh axis runs over, the one named last changes fastest.
Arguments:
- grads: float32 [768, 2304, 128], P(('dp', 'fsdp')), may hold values from -2.5 to 2.5
- last_peak: float32 [2304], replicated, may hold values from 0.05 to 0.8
- master: float32 [2304, 128], P(('dp', 'fsdp')), may hold values from -6 to 6
- moment1: float32 [2304, 128], P(('dp', 'fsdp')), may hold values from -6 to 6
- moment2: float32 [2304, 128], P(('dp', 'fsdp')), may hold values from 0.25 to 8
Outputs:
- new_master: float32 [2304, 128], P(('dp', 'fsdp'))
- new_moment1: float32 [2304, 128], P(('dp', 'fsdp'))
- new_moment2: float32 [2304, 128], P(('dp', 'fsdp'))
- weights: bfloat16 [2304, 128], replicated
- block_peak: float32 [2304], replicated
The draws below stay inside these ranges and needn't reach their ends.
All inputs are finite; a program needn't handle non-finite values.
Results may differ from the reference program's by a relative error of at most 0.0035.
Values may be sent and summed in bfloat16 or wider, within the bound.
A program may use at most 64 MiB of HBM per device.

```python
import math
import jax
import jax.numpy as jnp
from jax import lax

BLOCK = 128
STEP_COUNT = 10
REPLICAS = 768
BLOCKS = 2304


def strengthened(values, stream_key, source, target, parts, factor):
    def block_of(dim):
        return (jnp.arange(values.shape[dim]) // (values.shape[dim] // parts)).reshape((-1,) + (1,) * (values.ndim - 1 - dim))

    first = jax.random.permutation(stream_key, parts)[block_of(target)]
    other_side = (block_of(target) + parts // 2) % parts
    return jnp.where((block_of(source) == first) | (block_of(source) == other_side), factor * values, values)


def level_of(key, extent, split, low, high):
    factor_of, own = 1.0, jax.random.fold_in(key, 6)
    for axis_at, shards_of in split:
        draws = jnp.exp(jax.random.uniform(jax.random.fold_in(own, axis_at), (shards_of,), jnp.float32, low / len(split), high / len(split)))
        factor_of = factor_of * jnp.repeat(draws, extent[axis_at] // shards_of).reshape([-1 if axis == axis_at else 1 for axis in range(len(extent))])
    return factor_of


def scatter_about(own_key, extent, spread, reach, shards=(), kind=jnp.bfloat16):
    drawn = spread * jax.random.normal(own_key, extent, jnp.float32)
    if shards:
        drawn = drawn * level_of(own_key, extent, shards, -0.22, 0.18)
    return jnp.clip(drawn, -reach, reach).astype(kind)


def gaussian_with(own_key, shape, width, most, cuts, heavy, held_as=jnp.bfloat16):
    entries = width * jax.random.normal(own_key, shape, jnp.float32)
    if cuts:
        entries = entries * level_of(own_key, shape, cuts, -0.22, 0.18)
    return jnp.clip(strengthened(entries, jax.random.fold_in(own_key, 3), *heavy), -most, most).astype(held_as)


def setup_inputs(seed: int = 0) -> dict:
    seeds = jax.random.split(jax.random.key(seed), 6)
    return {
        "grads": gaussian_with(seeds[0], (REPLICAS, BLOCKS, BLOCK), 0.1, 2.5, ((0, 768),), (0, 1, 768, 6.0), jnp.float32),
        "last_peak": jnp.clip(jnp.exp(jax.random.uniform(seeds[1], (BLOCKS,), jnp.float32, math.log(0.05), math.log(0.8))), 0.05, 0.8),
        "master": scatter_about(seeds[2], (BLOCKS, BLOCK), 1.0, 6.0, ((0, 768),), jnp.float32),
        "moment1": scatter_about(seeds[3], (BLOCKS, BLOCK), 1.0, 6.0, ((0, 768),), jnp.float32),
        "moment2": jnp.clip(jnp.exp(math.log(8.0) - 3.465736 * jax.random.uniform(seeds[4], (BLOCKS, BLOCK), jnp.float32) ** level_of(seeds[4], (BLOCKS, BLOCK), ((0, 768),), -0.2, 0.2)), 0.25, 8.0),
    }


code_limit = 448.0
peak_floor = 0.05
beta_one = 0.9
beta_two = 0.95
learn_rate = 0.05
decay_rate = 0.1
epsilon = 1e-08

def quantize(rows, inverse):
    codes = jnp.clip(rows * inverse[:, None], -code_limit, code_limit).astype(jnp.bfloat16)
    return lax.optimization_barrier(codes).astype(jnp.float32)

def adamw(gradient, master, moment1, moment2):
    first = beta_one * moment1 + (1.0 - beta_one) * gradient
    second = beta_two * moment2 + (1.0 - beta_two) * gradient * gradient
    corrected_one = first / (1.0 - beta_one ** STEP_COUNT)
    corrected_two = second / (1.0 - beta_two ** STEP_COUNT)
    updated = master - learn_rate * (corrected_one / (jnp.sqrt(corrected_two) + epsilon) + decay_rate * master)
    return (updated, first, second)

def reference(grads, last_peak, master, moment1, moment2):

    def peak_step(carry, slab):
        return (jnp.maximum(carry, lax.optimization_barrier(jnp.max(jnp.abs(slab), axis=1))), None)
    peak, unused = lax.scan(peak_step, jnp.zeros((grads.shape[1],), jnp.float32), grads)
    floored = jnp.maximum(last_peak, peak_floor)
    inverse = code_limit / floored
    scale = floored / code_limit

    def add_step(total, slab):
        return (total + quantize(slab, inverse), None)
    summed, unused = lax.scan(add_step, jnp.zeros(grads.shape[1:], jnp.float32), grads)
    gradient = summed * scale[:, None]
    updated, first, second = adamw(gradient, master, moment1, moment2)
    return (updated, first, second, updated.astype(jnp.bfloat16), peak)
```

```python
import functools

import jax
import jax.numpy as jnp
from jax import lax
from jax.experimental import pallas as pl
from jax.experimental.pallas import tpu as pltpu
from jax.sharding import Mesh
from jax.sharding import PartitionSpec as P

STEP_COUNT = 10
AXES = ("dp_0", "dp_1", "dp_2", "fsdp")
MESH = pl.DeviceIdType.MESH

code_limit = 448.0
peak_floor = 0.05
beta_one = 0.9
beta_two = 0.95
learn_rate = 0.05
decay_rate = 0.1
epsilon = 1e-08

X, Y, C, Z = 4, 8, 2, 12
ROWS, WIDTH = 2304, 128
PIECE = ROWS // (X * C)
GROUP = ROWS // (X * Y)
SHARE = GROUP // C
OWNED = SHARE // Z
LANE_ROWS = ROWS // WIDTH
CHUNKS = 9


def adamw(gradient, master, moment1, moment2):
    first = beta_one * moment1 + (1.0 - beta_one) * gradient
    second = beta_two * moment2 + (1.0 - beta_two) * gradient * gradient
    corrected_one = first / (1.0 - beta_one**STEP_COUNT)
    corrected_two = second / (1.0 - beta_two**STEP_COUNT)
    updated = master - learn_rate * (
        corrected_one / (jnp.sqrt(corrected_two) + epsilon) + decay_rate * master
    )
    return (updated, first, second)


def kernel(
    grads, last_peak, master, moment1, moment2,
    out_master, out_first, out_second, weights, out_peak,
    g, lp, state, stepped, codes, r1, pk1, rp1, t1, s1, p1, r2, rp2, s2, r3, p3, rp3,
    w3, gz, a36, ay, gy, rp4, t288, wb, pg, rp5, peak_lanes,
    load_sem, small_sem, out_sem,
    ss1, rs1, sp1, rps1, ss2, rs2, sp2, rps2, ss3, rs3, sp3, rps3,
    sz, rz, sy, ry, sp4, rps4, sx, rx, sp5, rps5, sd, rd, so,
):
    x, y, c, z = (lax.axis_index(a) for a in AXES)
    mine = 2 * x + c
    half = y // 4
    inside = lax.rem(y, 4)

    def at(xx=None, yy=None, cc=None, zz=None):
        where = {"dp_0": xx, "dp_1": yy, "dp_2": cc, "fsdp": zz}
        return {k: v for k, v in where.items() if v is not None}

    def remote(src, dst, send, recv, where):
        return pltpu.make_async_remote_copy(
            src_ref=src, dst_ref=dst, send_sem=send, recv_sem=recv, device_id=where, device_id_type=MESH
        )

    barrier = pltpu.get_barrier_semaphore()
    for d in range(1, Z):
        pl.semaphore_signal(barrier, inc=1, device_id=at(zz=lax.rem(z + d, Z)), device_id_type=MESH)
    for d in range(1, Y):
        for cc in range(C):
            pl.semaphore_signal(barrier, inc=1, device_id=at(yy=lax.rem(y + d, Y), cc=cc), device_id_type=MESH)
    for d in range(1, X):
        for cc in range(C):
            pl.semaphore_signal(barrier, inc=1, device_id=at(xx=lax.rem(x + d, X), cc=cc), device_id_type=MESH)
    pl.semaphore_signal(barrier, inc=1, device_id=at(cc=1 - c), device_id_type=MESH)

    step_rows = ROWS // CHUNKS
    lp_copy = pltpu.make_async_copy(last_peak, lp, small_sem.at[0])
    lp_copy.start()
    loads = [
        pltpu.make_async_copy(
            grads.at[pl.ds(i * step_rows, step_rows)], g.at[pl.ds(i * step_rows, step_rows)], load_sem.at[i]
        )
        for i in range(CHUNKS)
    ]
    for copy in loads:
        copy.start()
    state_copies = [
        pltpu.make_async_copy(src, state.at[i], small_sem.at[1 + i])
        for i, src in enumerate((master, moment1, moment2))
    ]
    for copy in state_copies:
        copy.start()
    lp_copy.wait()

    square = (WIDTH, WIDTH)
    row_at = lax.broadcasted_iota(jnp.int32, square, 0)
    lane_at = lax.broadcasted_iota(jnp.int32, square, 1)
    for i in range(CHUNKS):
        loads[i].wait()
        for j in range(step_rows // WIDTH):
            r = i * (step_rows // WIDTH) + j
            rows = pl.ds(r * WIDTH, WIDTH)
            inverse = code_limit / jnp.maximum(lp[pl.ds(r, 1), :], peak_floor)
            spread = jnp.where(row_at == lane_at, jnp.broadcast_to(inverse, square), 0.0)
            column = jnp.sum(spread, axis=1, keepdims=True)
            scaled = g[rows, :] * column
            codes[rows, :] = jnp.clip(scaled, -code_limit, code_limit).astype(jnp.bfloat16)

    tall = (GROUP, WIDTH)
    tall_row = lax.broadcasted_iota(jnp.int32, tall, 0)
    tall_lane = lax.broadcasted_iota(jnp.int32, tall, 1)

    for k in range(X * C):
        for i in range(4):
            rows = pl.ds((4 * k + i) * GROUP, GROUP)
            top = jnp.max(jnp.abs(g[rows, :]), axis=1, keepdims=True)
            laid = jnp.where(tall_row == tall_lane, jnp.broadcast_to(top, tall), 0.0)
            pk1[k, i : i + 1, :] = jnp.max(laid, axis=0, keepdims=True)

    first_row = (((x * Y + y) * C + c) * Z + z) * OWNED
    flat = lax.broadcasted_iota(jnp.int32, (LANE_ROWS, WIDTH), 0) * WIDTH + lax.broadcasted_iota(
        jnp.int32, (LANE_ROWS, WIDTH), 1
    )
    own_row = lax.broadcasted_iota(jnp.int32, (OWNED, WIDTH), 0)
    all_scales = jnp.maximum(lp[...], peak_floor) / code_limit
    scale = jnp.zeros((OWNED, WIDTH), jnp.float32)
    for j in range(OWNED):
        one = jnp.sum(jnp.where(flat == first_row + j, all_scales, 0.0), axis=(0, 1), keepdims=True)
        scale = jnp.where(own_row == j, jnp.broadcast_to(one, scale.shape), scale)

    pl.semaphore_wait(barrier, (Z - 1) + (Y - 1) * C + (X - 1) * C + 1)

    def code_rows(k):
        return codes.at[pl.ds(pl.multiple_of(k * PIECE, 16), PIECE)]

    sent1 = []
    for d in (4, 5, 3, 6, 2, 7, 1):
        k = lax.rem(mine + d, X * C)
        where = at(xx=k // 2, cc=lax.rem(k, 2))
        sent1.append(remote(code_rows(k), r1.at[mine], ss1.at[d], rs1.at[mine], where))
        sent1.append(remote(pk1.at[k], rp1.at[mine], sp1.at[d], rps1.at[mine], where))
    for copy in sent1:
        copy.start()
    for d in range(1, X * C):
        k = lax.rem(mine + d, X * C)
        remote(r1.at[k], r1.at[k], ss1.at[d], rs1.at[k], at(cc=1 - c)).wait_recv()

    block = 48
    for b in range(PIECE // block):
        own = codes[pl.ds(pl.multiple_of(mine * PIECE + b * block, 16), block), :]
        total = own.astype(jnp.float32)
        for d in range(1, X * C):
            k = lax.rem(mine + d, X * C)
            total = total + r1[k, pl.ds(b * block, block), :].astype(jnp.float32)
        t1[pl.ds(b * block, block), :] = total
    for m in range(8):
        s1[m] = t1[pl.ds(m * SHARE, SHARE), :]

    def to_y(d, cc):
        yy = 4 * c + lax.rem(inside + d, 4)
        m = 2 * lax.rem(inside + d, 4) + cc
        return remote(s1.at[m], r2.at[y], ss2.at[2 * d + cc], rs2.at[y], at(yy=yy, cc=cc))

    def peak_to_y(d, cc):
        yy = 4 * c + lax.rem(inside + d, 4)
        return remote(
            p1.at[lax.rem(inside + d, 4)], rp2.at[y], sp2.at[2 * d + cc], rps2.at[y], at(yy=yy, cc=cc)
        )

    for d in (2, 3, 1):
        for cc in range(C):
            to_y(d, cc).start()
    other = 1 - c

    def own_y(make, sems):
        yy = 4 * c + inside
        return make, sems, yy

    def to_y0(cc, index):
        yy = 4 * c + inside
        return remote(s1.at[2 * inside + cc], r2.at[y], ss2.at[index], rs2.at[y], at(yy=yy, cc=cc))

    def peak_to_y0(cc, index):
        yy = 4 * c + inside
        return remote(p1.at[inside], rp2.at[y], sp2.at[index], rps2.at[y], at(yy=yy, cc=cc))

    to_y0(other, 0).start()

    @pl.when(half != c)
    def _():
        to_y0(c, 1).start()

    @pl.when(half == c)
    def _():
        r2[y] = s1[2 * inside + c]

    for d in range(1, X * C):
        k = lax.rem(mine + d, X * C)
        remote(rp1.at[k], rp1.at[k], sp1.at[d], rps1.at[k], at(cc=1 - c)).wait_recv()
    top = pk1[mine]
    for d in range(1, X * C):
        top = jnp.maximum(top, rp1[lax.rem(mine + d, X * C)])
    for i in range(4):
        p1[i] = top[i : i + 1, :]
    for d in (2, 3, 1):
        for cc in range(C):
            peak_to_y(d, cc).start()
    peak_to_y0(other, 0).start()

    @pl.when(half != c)
    def _():
        peak_to_y0(c, 1).start()

    @pl.when(half == c)
    def _():
        rp2[y] = p1[inside]

    for d in range(1, Y):
        yy = lax.rem(y + d, Y)
        remote(r2.at[yy], r2.at[yy], ss2.at[0], rs2.at[yy], at(cc=1 - c)).wait_recv()

    @pl.when(half != c)
    def _():
        remote(r2.at[y], r2.at[y], ss2.at[0], rs2.at[y], at(cc=1 - c)).wait_recv()

    total = r2[0]
    for i in range(1, Y):
        total = total + r2[i]
    for i in range(Z):
        s2[i] = total[i * OWNED : (i + 1) * OWNED, :]

    def to_z(d):
        zz = lax.rem(z + d, Z)
        return remote(s2.at[zz], r3.at[z], ss3.at[d], rs3.at[z], at(zz=zz))

    far_z = (6, 7, 5, 8, 4, 9, 3, 10, 2, 11, 1)
    for d in far_z:
        to_z(d).start()

    for d in range(1, Y):
        yy = lax.rem(y + d, Y)
        remote(rp2.at[yy], rp2.at[yy], sp2.at[0], rps2.at[yy], at(cc=1 - c)).wait_recv()

    @pl.when(half != c)
    def _():
        remote(rp2.at[y], rp2.at[y], sp2.at[0], rps2.at[y], at(cc=1 - c)).wait_recv()

    top = rp2[0]
    for i in range(1, Y):
        top = jnp.maximum(top, rp2[i])
    p3[...] = top

    def peak_to_z(d):
        return remote(p3, rp3.at[z], sp3.at[d], rps3.at[z], at(zz=lax.rem(z + d, Z)))

    for d in far_z:
        peak_to_z(d).start()

    for copy in state_copies:
        copy.wait()
    for d in range(1, Z):
        zz = lax.rem(z + d, Z)
        remote(r3.at[zz], r3.at[zz], ss3.at[d], rs3.at[zz], at(zz=zz)).wait_recv()
    total = s2[z]
    for d in range(1, Z):
        total = total + r3[lax.rem(z + d, Z)]
    gradient = total * scale
    updated, first, second = adamw(gradient, state[0], state[1], state[2])
    w3[...] = updated.astype(jnp.bfloat16).astype(jnp.float32)
    stepped[0] = updated
    stepped[1] = first
    stepped[2] = second

    def give_z(d):
        return remote(w3, gz.at[z], sz.at[d], rz.at[z], at(zz=lax.rem(z + d, Z)))

    for d in far_z:
        give_z(d).start()
    gz[z] = w3[...]
    step_outs = [
        pltpu.make_async_copy(stepped.at[i], dst, out_sem.at[i])
        for i, dst in enumerate((out_master, out_first, out_second))
    ]
    for copy in step_outs:
        copy.start()

    for d in range(1, Z):
        zz = lax.rem(z + d, Z)
        remote(rp3.at[zz], rp3.at[zz], sp3.at[d], rps3.at[zz], at(zz=zz)).wait_recv()
    top = p3[...]
    for d in range(1, Z):
        top = jnp.maximum(top, rp3[lax.rem(z + d, Z)])
    rp4[y] = top

    def peak_give_y(d):
        return remote(rp4.at[y], rp4.at[y], sp4.at[d], rps4.at[y], at(yy=lax.rem(y + d, Y)))

    far_y = (4, 5, 3, 6, 2, 7, 1)
    for d in far_y:
        peak_give_y(d).start()

    for d in range(1, Z):
        zz = lax.rem(z + d, Z)
        remote(gz.at[zz], gz.at[zz], sz.at[d], rz.at[zz], at(zz=zz)).wait_recv()
    for i in range(Z):
        a36[pl.ds(i * OWNED, OWNED), :] = gz[i]
    ay[...] = a36[...].astype(jnp.bfloat16)

    slot = 2 * inside + c

    def give_y(d):
        return remote(ay, gy.at[slot], sy.at[d], ry.at[slot], at(yy=lax.rem(y + d, Y), cc=half))

    for d in far_y:
        give_y(d).start()

    @pl.when(half != c)
    def _():
        remote(ay, gy.at[slot], sy.at[0], ry.at[slot], at(cc=half)).start()

    @pl.when(half == c)
    def _():
        gy[slot] = ay[...]

    for d in range(1, Y):
        yy = lax.rem(y + d, Y)
        remote(rp4.at[yy], rp4.at[yy], sp4.at[d], rps4.at[yy], at(yy=yy)).wait_recv()
    for i in range(Y):
        pg[i : i + 1, :] = rp4[i]

    def peak_give_x(d):
        return remote(pg, rp5.at[x], sp5.at[d], rps5.at[x], at(xx=lax.rem(x + d, X)))

    for d in (2, 3, 1):
        peak_give_x(d).start()
    rp5[x] = pg[...]

    for m in range(8):
        @pl.when((half != c) | (m != slot))
        def _():
            remote(gy.at[m], gy.at[m], sy.at[0], ry.at[m], at(cc=1 - c)).wait_recv()

    for m in range(8):
        t288[pl.ds(m * SHARE, SHARE), :] = gy[m].astype(jnp.float32)
    wb[mine] = t288[...].astype(jnp.bfloat16)

    def out_rows(k):
        return weights.at[pl.ds(pl.multiple_of(k * PIECE, 16), PIECE)]

    def give_x(d):
        return remote(wb.at[mine], wb.at[mine], sx.at[d], rx.at[mine], at(xx=lax.rem(x + d, X)))

    def give_core(d):
        k = 2 * lax.rem(x + d, X) + c
        return remote(wb.at[k], out_rows(k), sd.at[d], rd.at[d], at(cc=1 - c))

    def keep(d):
        k = 2 * lax.rem(x + d, X) + c
        return pltpu.make_async_copy(wb.at[k], out_rows(k), so.at[d])

    for d in (2, 3, 1):
        give_x(d).start()
    give_core(0).start()
    keep(0).start()

    for d in range(1, X):
        xx = lax.rem(x + d, X)
        remote(rp5.at[xx], rp5.at[xx], sp5.at[d], rps5.at[xx], at(xx=xx)).wait_recv()
    lane_of = lax.broadcasted_iota(jnp.int32, (1, WIDTH), 1)
    for j in range(LANE_ROWS):
        line = jnp.zeros((1, WIDTH), jnp.float32)
        for n in range(X * Y):
            lo = GROUP * n - WIDTH * j
            if lo >= WIDTH or lo + GROUP <= 0:
                continue
            row = rp5[n // Y, n % Y : n % Y + 1, :]
            if lo % WIDTH:
                row = pltpu.roll(row, lo % WIDTH, 1)
            line = jnp.where((lane_of >= lo) & (lane_of < lo + GROUP), row, line)
        peak_lanes[j : j + 1, :] = line
    peak_out = pltpu.make_async_copy(peak_lanes, out_peak, out_sem.at[3])
    peak_out.start()

    for d in (1, 3, 2):
        xx = lax.rem(x + d, X)
        k = 2 * xx + c
        remote(wb.at[k], wb.at[k], sx.at[d], rx.at[k], at(xx=xx)).wait_recv()
        give_core(d).start()
        keep(d).start()

    for copy in sent1:
        copy.wait_send()
    for d in (2, 3, 1):
        for cc in range(C):
            to_y(d, cc).wait_send()
            peak_to_y(d, cc).wait_send()
    to_y0(other, 0).wait_send()
    peak_to_y0(other, 0).wait_send()

    @pl.when(half != c)
    def _():
        to_y0(c, 1).wait_send()
        peak_to_y0(c, 1).wait_send()
        remote(ay, gy.at[slot], sy.at[0], ry.at[slot], at(cc=half)).wait_send()

    for d in far_z:
        to_z(d).wait_send()
        peak_to_z(d).wait_send()
        give_z(d).wait_send()
    for d in far_y:
        peak_give_y(d).wait_send()
        give_y(d).wait_send()
    for d in (1, 2, 3):
        peak_give_x(d).wait_send()
        give_x(d).wait_send()
    for copy in step_outs:
        copy.wait()
    peak_out.wait()
    for d in range(X):
        give_core(d).wait_send()
        keep(d).wait()
    for d in range(X):
        k = 2 * lax.rem(x + d, X) + 1 - c
        remote(wb.at[k], out_rows(k), sd.at[d], rd.at[d], at(cc=1 - c)).wait_recv()


def body(grads, last_peak, master, moment1, moment2):
    f32, bf16 = jnp.float32, jnp.bfloat16
    vmem = lambda *shape, dtype=f32: pltpu.VMEM(shape, dtype)
    dma = lambda n: pltpu.SemaphoreType.DMA((n,))
    own = jax.ShapeDtypeStruct((OWNED, WIDTH), f32)
    updated, first, second, weights, peak = pl.pallas_call(
        kernel,
        out_shape=[
            own, own, own,
            jax.ShapeDtypeStruct((ROWS, WIDTH), bf16),
            jax.ShapeDtypeStruct((LANE_ROWS, WIDTH), f32),
        ],
        in_specs=[pl.BlockSpec(memory_space=pl.ANY)] * 5,
        out_specs=[pl.BlockSpec(memory_space=pl.ANY)] * 5,
        scratch_shapes=[
            vmem(ROWS, WIDTH),
            vmem(LANE_ROWS, WIDTH),
            vmem(3, OWNED, WIDTH),
            vmem(3, OWNED, WIDTH),
            vmem(ROWS, WIDTH, dtype=bf16),
            vmem(X * C, PIECE, WIDTH, dtype=bf16),
            vmem(X * C, 4, WIDTH),
            vmem(X * C, 4, WIDTH),
            vmem(PIECE, WIDTH),
            vmem(8, SHARE, WIDTH),
            vmem(4, 1, WIDTH),
            vmem(Y, SHARE, WIDTH),
            vmem(Y, 1, WIDTH),
            vmem(Z, OWNED, WIDTH),
            vmem(Z, OWNED, WIDTH),
            vmem(1, WIDTH),
            vmem(Z, 1, WIDTH),
            vmem(OWNED, WIDTH),
            vmem(Z, OWNED, WIDTH),
            vmem(SHARE, WIDTH),
            vmem(SHARE, WIDTH, dtype=bf16),
            vmem(8, SHARE, WIDTH, dtype=bf16),
            vmem(Y, 1, WIDTH),
            vmem(PIECE, WIDTH),
            vmem(X * C, PIECE, WIDTH, dtype=bf16),
            vmem(Y, WIDTH),
            vmem(X, Y, WIDTH),
            vmem(LANE_ROWS, WIDTH),
            dma(CHUNKS), dma(4), dma(4),
            dma(8), dma(8), dma(8), dma(8),
            dma(8), dma(8), dma(8), dma(8),
            dma(Z), dma(Z), dma(Z), dma(Z),
            dma(Z), dma(Z), dma(8), dma(8), dma(8), dma(8),
            dma(X), dma(8), dma(X), dma(X), dma(X), dma(X), dma(X),
        ],
        compiler_params=pltpu.CompilerParams(collective_id=0, has_side_effects=True),
    )(grads.reshape(ROWS, WIDTH), last_peak.reshape(LANE_ROWS, WIDTH), master, moment1, moment2)
    return (updated, first, second, weights, peak.reshape(ROWS))


def solution(mesh):
    torus = Mesh(mesh.devices.reshape(X, Y, C, Z), AXES)
    in_specs = (P(AXES, None, None), P(), P(AXES, None), P(AXES, None), P(AXES, None))
    out_specs = (P(AXES, None), P(AXES, None), P(AXES, None), P(), P())
    return jax.shard_map(body, mesh=torus, in_specs=in_specs, out_specs=out_specs, check_vma=False)
```

```python
import functools

import jax
import jax.numpy as jnp
from jax import lax
from jax.experimental import pallas as pl
from jax.experimental.pallas import tpu as pltpu
from jax.sharding import Mesh
from jax.sharding import PartitionSpec as P

STEP_COUNT = 10
AXES = ("dp_0", "dp_1", "dp_2", "fsdp")
MESH = pl.DeviceIdType.MESH

code_limit = 448.0
peak_floor = 0.05
beta_one = 0.9
beta_two = 0.95
learn_rate = 0.05
decay_rate = 0.1
epsilon = 1e-08

X, Y, C, Z = 4, 8, 2, 12
ROWS, WIDTH = 2304, 128
PIECE = ROWS // (X * C)
GROUP = ROWS // (X * Y)
SHARE = GROUP // C
OWNED = SHARE // Z
LANE_ROWS = ROWS // WIDTH


def adamw(gradient, master, moment1, moment2):
    first = beta_one * moment1 + (1.0 - beta_one) * gradient
    second = beta_two * moment2 + (1.0 - beta_two) * gradient * gradient
    corrected_one = first / (1.0 - beta_one**STEP_COUNT)
    corrected_two = second / (1.0 - beta_two**STEP_COUNT)
    updated = master - learn_rate * (
        corrected_one / (jnp.sqrt(corrected_two) + epsilon) + decay_rate * master
    )
    return (updated, first, second)


_cur = [None]


def phase(name):
    if _cur[0] is not None:
        _cur[0].__exit__(None, None, None)
    _cur[0] = None
    if name:
        _cur[0] = jax.named_scope(name)
        _cur[0].__enter__()


def kernel(
    grads, last_peak, master, moment1, moment2,
    stepped, wb, peak_lanes,
    g, lp, inv, state, codes, r1, pk1, rp1, t1, s1, p1, r2, rp2, s2, r3, p3, rp3,
    w3, gz, a36, ay, gy, rp4, t288, pg, rp5,
    up, down, load_sem, small_sem, sem,
    rx,
):
    x, y, c, z = (lax.axis_index(a) for a in AXES)
    mine = 2 * x + c
    half = y // 4
    inside = lax.rem(y, 4)
    far_z = (6, 7, 5, 8, 4, 9, 3, 10, 2, 11, 1)
    far_y = (4, 5, 3, 6, 2, 7, 1)
    far_k = (4, 5, 3, 6, 2, 7, 1)
    count = [0]

    def new_sem():
        count[0] += 1
        return sem.at[count[0] - 1]

    def at(xx=None, yy=None, cc=None, zz=None):
        where = {"dp_0": xx, "dp_1": yy, "dp_2": cc, "fsdp": zz}
        return {k: v for k, v in where.items() if v is not None}

    def signal(semaphore, **where):
        pl.semaphore_signal(semaphore, inc=1, device_id=at(**where), device_id_type=MESH)

    def remote(src, dst, send, recv, where):
        return pltpu.make_async_remote_copy(
            src_ref=src, dst_ref=dst, send_sem=send, recv_sem=recv, device_id=where, device_id_type=MESH
        )

    def arrived(ref, semaphore):
        remote(ref, ref, semaphore, semaphore, at(cc=1 - c)).wait_recv()

    def departed(ref, semaphore):
        remote(ref, ref, semaphore, semaphore, at(cc=1 - c)).wait_send()

    phase("a_signal")
    barrier = pltpu.get_barrier_semaphore()
    signal(barrier, zz=lax.rem(z + 1, Z))
    signal(barrier, zz=lax.rem(z + Z - 1, Z))
    for d in far_y:
        for cc in range(C):
            signal(barrier, yy=lax.rem(y + d, Y), cc=cc)
    for d in (2, 3, 1):
        for cc in range(C):
            signal(barrier, xx=lax.rem(x + d, X), cc=cc)
    signal(barrier, cc=1 - c)

    phase("b_load")
    lp_copy = pltpu.make_async_copy(last_peak, lp, small_sem.at[0])
    lp_copy.start()

    def rows_of(k):
        return pl.ds(pl.multiple_of(k * PIECE, 32), PIECE)

    order = [lax.rem(mine + d, X * C) for d in far_k + (0,)]
    loads = [
        pltpu.make_async_copy(grads.at[rows_of(k)], g.at[rows_of(k)], load_sem.at[i])
        for i, k in enumerate(order)
    ]
    for copy in loads:
        copy.start()
    state_copies = [
        pltpu.make_async_copy(src, state.at[i], small_sem.at[1 + i])
        for i, src in enumerate((master, moment1, moment2))
    ]
    for copy in state_copies:
        copy.start()
    lp_copy.wait()

    phase("c_inverse")
    square = (WIDTH, WIDTH)
    row_at = lax.broadcasted_iota(jnp.int32, square, 0)
    lane_at = lax.broadcasted_iota(jnp.int32, square, 1)
    for r in range(LANE_ROWS):
        inverse = code_limit / jnp.maximum(lp[pl.ds(r, 1), :], peak_floor)
        spread = jnp.where(row_at == lane_at, jnp.broadcast_to(inverse, square), 0.0)
        column = jnp.sum(spread, axis=1, keepdims=True)
        inv[pl.ds(r * WIDTH, WIDTH), :] = jnp.broadcast_to(column, square)

    def encode(i):
        loads[i].wait()
        rows = rows_of(order[i])
        codes[rows, :] = jnp.clip(g[rows, :] * inv[rows, :], -code_limit, code_limit).astype(jnp.bfloat16)

    phase("d_first")
    encode(0)

    phase("e_barrier")
    pl.semaphore_wait(barrier, 2 + (Y - 1) * C + (X - 1) * C + 1)

    phase("f_send1")
    sent_codes, got_codes, sent_pk1, got_pk1 = (new_sem() for _ in range(4))
    for i, k in enumerate(order[:-1]):
        if i:
            encode(i)
        remote(codes.at[rows_of(k)], r1.at[mine], sent_codes, got_codes, at(xx=k // 2, cc=lax.rem(k, 2))).start()
    encode(X * C - 1)

    phase("g_zround")

    def tell(upwards, downwards):
        signal(up, zz=lax.rem(z + 1, Z))
        signal(down, zz=lax.rem(z + Z - 1, Z))

    def hear():
        pl.semaphore_wait(up, 1)
        pl.semaphore_wait(down, 1)

    tell(up, down)

    phase("h_peaks")
    tall = (GROUP, WIDTH)
    tall_row = lax.broadcasted_iota(jnp.int32, tall, 0)
    tall_lane = lax.broadcasted_iota(jnp.int32, tall, 1)
    for k in range(X * C):
        for i in range(4):
            rows = pl.ds((4 * k + i) * GROUP, GROUP)
            top = jnp.max(jnp.abs(g[rows, :]), axis=1, keepdims=True)
            laid = jnp.where(tall_row == tall_lane, jnp.broadcast_to(top, tall), 0.0)
            pk1[k, i : i + 1, :] = jnp.max(laid, axis=0, keepdims=True)
    for k in order[:-1]:
        remote(pk1.at[k], rp1.at[mine], sent_pk1, got_pk1, at(xx=k // 2, cc=lax.rem(k, 2))).start()

    phase("i_zround")
    for _ in range(Z // 2 - 2):
        hear()
        tell(up, down)
    hear()

    phase("j_scale")
    first_row = (((x * Y + y) * C + c) * Z + z) * OWNED
    flat = lax.broadcasted_iota(jnp.int32, (LANE_ROWS, WIDTH), 0) * WIDTH + lax.broadcasted_iota(
        jnp.int32, (LANE_ROWS, WIDTH), 1
    )
    own_row = lax.broadcasted_iota(jnp.int32, (OWNED, WIDTH), 0)
    all_scales = jnp.maximum(lp[...], peak_floor) / code_limit
    scale = jnp.zeros((OWNED, WIDTH), jnp.float32)
    for j in range(OWNED):
        one = jnp.sum(jnp.where(flat == first_row + j, all_scales, 0.0), axis=(0, 1), keepdims=True)
        scale = jnp.where(own_row == j, jnp.broadcast_to(one, scale.shape), scale)

    phase("k_wait1")
    arrived(r1.at[pl.ds(0, X * C - 1)], got_codes)

    phase("l_sum1")
    block = 48
    for b in range(PIECE // block):
        own = codes[pl.ds(pl.multiple_of(mine * PIECE + b * block, 16), block), :]
        total = own.astype(jnp.float32)
        for d in range(1, X * C):
            k = lax.rem(mine + d, X * C)
            total = total + r1[k, pl.ds(b * block, block), :].astype(jnp.float32)
        t1[pl.ds(b * block, block), :] = total
    for m in range(8):
        s1[m] = t1[pl.ds(m * SHARE, SHARE), :]

    phase("m_send2")
    sent2, got2, sent_p2, got_p2 = (new_sem() for _ in range(4))
    local = half == c

    def to_y(start, source, landing, semaphores):
        for d in (2, 3, 1):
            for cc in range(C):
                i = lax.rem(inside + d, 4)
                start(source(i, cc), landing, semaphores, at(yy=4 * c + i, cc=cc))
        start(source(inside, 1 - c), landing, semaphores, at(yy=4 * c + inside, cc=1 - c))

        @pl.when(jnp.logical_not(local))
        def _():
            start(source(inside, c), landing, semaphores, at(yy=4 * c + inside, cc=c))

    def start(src, dst, semaphores, where):
        remote(src, dst, *semaphores, where).start()

    def finish(kind, ref, semaphore):
        @pl.when(local)
        def _():
            kind(ref.at[pl.ds(0, 7)], semaphore)

        @pl.when(jnp.logical_not(local))
        def _():
            kind(ref, semaphore)

    to_y(start, lambda i, cc: s1.at[2 * i + cc], r2.at[y], (sent2, got2))

    @pl.when(local)
    def _():
        r2[y] = s1[2 * inside + c]

    phase("n_peak1")
    arrived(rp1.at[pl.ds(0, X * C - 1)], got_pk1)
    top = pk1[mine]
    for d in range(1, X * C):
        top = jnp.maximum(top, rp1[lax.rem(mine + d, X * C)])
    for i in range(4):
        p1[i] = top[i : i + 1, :]
    to_y(start, lambda i, cc: p1.at[i], rp2.at[y], (sent_p2, got_p2))

    @pl.when(local)
    def _():
        rp2[y] = p1[inside]

    phase("o_wait2")
    finish(arrived, r2, got2)
    phase("p_sum2")
    total = r2[0]
    for i in range(1, Y):
        total = total + r2[i]
    for i in range(Z):
        s2[i] = total[i * OWNED : (i + 1) * OWNED, :]

    phase("q_send3")
    sent3, got3, sent_p3, got_p3 = (new_sem() for _ in range(4))
    for d in far_z:
        zz = lax.rem(z + d, Z)
        start(s2.at[zz], r3.at[z], (sent3, got3), at(zz=zz))

    phase("r_peak2")
    finish(arrived, rp2, got_p2)
    top = rp2[0]
    for i in range(1, Y):
        top = jnp.maximum(top, rp2[i])
    p3[...] = top
    for d in far_z:
        start(p3, rp3.at[z], (sent_p3, got_p3), at(zz=lax.rem(z + d, Z)))

    for copy in state_copies:
        copy.wait()
    phase("s_wait3")
    arrived(r3.at[pl.ds(0, Z - 1)], got3)
    phase("t_adam")
    total = s2[z]
    for d in range(1, Z):
        total = total + r3[lax.rem(z + d, Z)]
    gradient = total * scale
    updated, first, second = adamw(gradient, state[0], state[1], state[2])
    w3[...] = updated.astype(jnp.bfloat16).astype(jnp.float32)

    phase("u_givez")
    sent_z, got_z = new_sem(), new_sem()
    for d in far_z:
        start(w3, gz.at[z], (sent_z, got_z), at(zz=lax.rem(z + d, Z)))
    gz[z] = w3[...]
    stepped[0] = updated
    stepped[1] = first
    stepped[2] = second

    phase("v_peak3")
    arrived(rp3.at[pl.ds(0, Z - 1)], got_p3)
    top = p3[...]
    for d in range(1, Z):
        top = jnp.maximum(top, rp3[lax.rem(z + d, Z)])
    rp4[y] = top
    sent_p4, got_p4 = new_sem(), new_sem()
    for d in far_y:
        start(rp4.at[y], rp4.at[y], (sent_p4, got_p4), at(yy=lax.rem(y + d, Y)))

    phase("w_waitgz")
    arrived(gz.at[pl.ds(0, Z - 1)], got_z)
    phase("x_asm36")
    for i in range(Z):
        a36[pl.ds(i * OWNED, OWNED), :] = gz[i]
    ay[...] = a36[...].astype(jnp.bfloat16)

    phase("y_givey")
    slot = 2 * inside + c
    sent_y, got_y = new_sem(), new_sem()
    for d in far_y:
        start(ay, gy.at[slot], (sent_y, got_y), at(yy=lax.rem(y + d, Y), cc=half))

    @pl.when(jnp.logical_not(local))
    def _():
        start(ay, gy.at[slot], (sent_y, got_y), at(cc=half))

    @pl.when(local)
    def _():
        gy[slot] = ay[...]

    phase("z_peakx")
    arrived(rp4.at[pl.ds(0, Y - 1)], got_p4)
    for i in range(Y):
        pg[i : i + 1, :] = rp4[i]
    sent_p5, got_p5 = new_sem(), new_sem()
    for d in (2, 3, 1):
        start(pg, rp5.at[x], (sent_p5, got_p5), at(xx=lax.rem(x + d, X)))
    rp5[x] = pg[...]

    phase("za_waitgy")
    finish(arrived, gy, got_y)
    phase("zb_asm288")
    for m in range(8):
        t288[pl.ds(m * SHARE, SHARE), :] = gy[m].astype(jnp.float32)
    wb[rows_of(mine), :] = t288[...].astype(jnp.bfloat16)

    phase("zc_givex")
    sent_x, sent_core, got_core = (new_sem() for _ in range(3))
    own_piece = wb.at[rows_of(mine)]
    for d in (2, 3, 1):
        start(own_piece, own_piece, (sent_x, rx.at[x]), at(xx=lax.rem(x + d, X)))

    def give_core(xx):
        piece = wb.at[rows_of(2 * xx + c)]
        start(piece, piece, (sent_core, got_core), at(cc=1 - c))

    give_core(x)

    phase("zd_peaks")
    arrived(rp5.at[pl.ds(0, X - 1)], got_p5)
    lane_of = lax.broadcasted_iota(jnp.int32, (1, WIDTH), 1)
    for j in range(LANE_ROWS):
        line = jnp.zeros((1, WIDTH), jnp.float32)
        for n in range(X * Y):
            lo = GROUP * n - WIDTH * j
            if lo >= WIDTH or lo + GROUP <= 0:
                continue
            row = rp5[n // Y, n % Y : n % Y + 1, :]
            if lo % WIDTH:
                row = pltpu.roll(row, lo % WIDTH, 1)
            line = jnp.where((lane_of >= lo) & (lane_of < lo + GROUP), row, line)
        peak_lanes[j : j + 1, :] = line

    phase("ze_waitgx")
    for d in (1, 3, 2):
        xx = lax.rem(x + d, X)
        arrived(wb.at[rows_of(2 * xx + c)], rx.at[xx])
        give_core(xx)

    phase("zf_drain")
    departed(r1.at[pl.ds(0, X * C - 1)], sent_codes)
    departed(rp1.at[pl.ds(0, X * C - 1)], sent_pk1)
    finish(departed, r2, sent2)
    finish(departed, rp2, sent_p2)
    departed(r3.at[pl.ds(0, Z - 1)], sent3)
    departed(rp3.at[pl.ds(0, Z - 1)], sent_p3)
    departed(gz.at[pl.ds(0, Z - 1)], sent_z)
    departed(rp4.at[pl.ds(0, Y - 1)], sent_p4)
    finish(departed, gy, sent_y)
    departed(rp5.at[pl.ds(0, X - 1)], sent_p5)
    departed(r1.at[pl.ds(0, X - 1)], sent_x)
    departed(r1.at[pl.ds(0, X)], sent_core)
    arrived(r1.at[pl.ds(0, X)], got_core)
    phase(None)


SEMS = 24


def store(stepped, wb, peak_lanes, out_master, out_first, out_second, weights, out_peak, sem):
    copies = [pltpu.make_async_copy(wb, weights, sem.at[0])]
    for i, dst in enumerate((out_master, out_first, out_second)):
        copies.append(pltpu.make_async_copy(stepped.at[i], dst, sem.at[1 + i]))
    copies.append(pltpu.make_async_copy(peak_lanes, out_peak, sem.at[4]))
    for copy in copies:
        copy.start()
    for copy in copies:
        copy.wait()


def body(grads, last_peak, master, moment1, moment2):
    f32, bf16 = jnp.float32, jnp.bfloat16
    vmem = lambda *shape, dtype=f32: pltpu.VMEM(shape, dtype)
    dma = lambda n: pltpu.SemaphoreType.DMA((n,))
    own = jax.ShapeDtypeStruct((OWNED, WIDTH), f32)
    whole = jax.ShapeDtypeStruct((ROWS, WIDTH), bf16)
    lanes = jax.ShapeDtypeStruct((LANE_ROWS, WIDTH), f32)
    in_vmem = pl.BlockSpec(memory_space=pltpu.VMEM)
    anywhere = pl.BlockSpec(memory_space=pl.ANY)
    held = pl.pallas_call(
        kernel,
        out_shape=[jax.ShapeDtypeStruct((3, OWNED, WIDTH), f32), whole, lanes],
        in_specs=[pl.BlockSpec(memory_space=pltpu.HBM)] * 5,
        out_specs=[in_vmem] * 3,
        scratch_shapes=[
            vmem(ROWS, WIDTH),
            vmem(LANE_ROWS, WIDTH),
            vmem(ROWS, WIDTH),
            vmem(3, OWNED, WIDTH),
            vmem(ROWS, WIDTH, dtype=bf16),
            vmem(X * C, PIECE, WIDTH, dtype=bf16),
            vmem(X * C, 4, WIDTH),
            vmem(X * C, 4, WIDTH),
            vmem(PIECE, WIDTH),
            vmem(8, SHARE, WIDTH),
            vmem(4, 1, WIDTH),
            vmem(Y, SHARE, WIDTH),
            vmem(Y, 1, WIDTH),
            vmem(Z, OWNED, WIDTH),
            vmem(Z, OWNED, WIDTH),
            vmem(1, WIDTH),
            vmem(Z, 1, WIDTH),
            vmem(OWNED, WIDTH),
            vmem(Z, OWNED, WIDTH),
            vmem(SHARE, WIDTH),
            vmem(SHARE, WIDTH, dtype=bf16),
            vmem(8, SHARE, WIDTH, dtype=bf16),
            vmem(Y, 1, WIDTH),
            vmem(PIECE, WIDTH),
            vmem(Y, WIDTH),
            vmem(X, Y, WIDTH),
            pltpu.SemaphoreType.REGULAR,
            pltpu.SemaphoreType.REGULAR,
            dma(X * C), dma(4), dma(SEMS), dma(X),
        ],
        compiler_params=pltpu.CompilerParams(
            collective_id=0, has_side_effects=True, vmem_limit_bytes=16 * 2**20
        ),
    )(*(
        pltpu.with_memory_space_constraint(a, pltpu.HBM)
        for a in (grads.reshape(ROWS, WIDTH), last_peak.reshape(LANE_ROWS, WIDTH), master, moment1, moment2)
    ))
    updated, first, second, weights, peak = pl.pallas_call(
        store,
        out_shape=[own, own, own, whole, lanes],
        in_specs=[in_vmem] * 3,
        out_specs=[anywhere] * 5,
        scratch_shapes=[dma(5)],
        compiler_params=pltpu.CompilerParams(vmem_limit_bytes=8 * 2**20),
    )(*held)
    return (updated, first, second, weights, peak.reshape(ROWS))


def solution(mesh):
    torus = Mesh(mesh.devices.reshape(X, Y, C, Z), AXES)
    in_specs = (P(AXES, None, None), P(), P(AXES, None), P(AXES, None), P(AXES, None))
    out_specs = (P(AXES, None), P(AXES, None), P(AXES, None), P(), P())
    return jax.shard_map(body, mesh=torus, in_specs=in_specs, out_specs=out_specs, check_vma=False)
```

```python
import functools

import jax
import jax.numpy as jnp
from jax import lax
from jax.experimental import pallas as pl
from jax.experimental.pallas import tpu as pltpu
from jax.sharding import Mesh
from jax.sharding import PartitionSpec as P

STEP_COUNT = 10
AXES = ("dp_0", "dp_1", "dp_2", "fsdp")
MESH = pl.DeviceIdType.MESH

code_limit = 448.0
peak_floor = 0.05
beta_one = 0.9
beta_two = 0.95
learn_rate = 0.05
decay_rate = 0.1
epsilon = 1e-08

X, Y, C, Z = 4, 8, 2, 12
ROWS, WIDTH = 2304, 128
PIECE = ROWS // (X * C)
GROUP = ROWS // (X * Y)
SHARE = GROUP // C
OWNED = SHARE // Z
LANE_ROWS = ROWS // WIDTH
FIRST = 40
LAST = GROUP - FIRST
SPLIT = FIRST - SHARE
NEAR = 3


def adamw(gradient, master, moment1, moment2):
    first = beta_one * moment1 + (1.0 - beta_one) * gradient
    second = beta_two * moment2 + (1.0 - beta_two) * gradient * gradient
    corrected_one = first / (1.0 - beta_one**STEP_COUNT)
    corrected_two = second / (1.0 - beta_two**STEP_COUNT)
    updated = master - learn_rate * (
        corrected_one / (jnp.sqrt(corrected_two) + epsilon) + decay_rate * master
    )
    return (updated, first, second)


_cur = [None]


def phase(name):
    if _cur[0] is not None:
        _cur[0].__exit__(None, None, None)
    _cur[0] = None
    if name:
        _cur[0] = jax.named_scope(name)
        _cur[0].__enter__()


def kernel(
    grads, last_peak, master, moment1, moment2,
    stepped, wb, peak_lanes,
    g, lp, inv, state, codes_a, codes_b, r1a, r1b, pk1, rp1, s1a, s1b, s1c, p1, r2a, r2b, r2c, rp2, t36,
    s2, r3, p3, rp3, w3, gz, a36, ay, a4, b32, gya, gyb, rp4, t160, pg, rp5,
    up, down, load_sem, small_sem, sem, rxa, ryb,
):
    x, y, c, z = (lax.axis_index(a) for a in AXES)
    mine = 2 * x + c
    half = y // 4
    inside = lax.rem(y, 4)
    xhalf = x // 2
    xin = lax.rem(x, 2)
    first_core = c == 0
    last_core = c == 1
    local = half == c
    far_z = (6, 7, 5, 8, 4, 9, 3, 10, 2, 11, 1)
    far_y = (4, 5, 3, 6, 2, 7, 1)
    far_k = (4, 5, 3, 6, 2, 7, 1)
    count = [0]

    def new_sem():
        count[0] += 1
        return sem.at[count[0] - 1]

    def at(xx=None, yy=None, cc=None, zz=None):
        where = {"dp_0": xx, "dp_1": yy, "dp_2": cc, "fsdp": zz}
        return {k: v for k, v in where.items() if v is not None}

    def signal(semaphore, **where):
        pl.semaphore_signal(semaphore, inc=1, device_id=at(**where), device_id_type=MESH)

    def remote(src, dst, send, recv, where):
        return pltpu.make_async_remote_copy(
            src_ref=src, dst_ref=dst, send_sem=send, recv_sem=recv, device_id=where, device_id_type=MESH
        )

    def arrived(ref, semaphore):
        remote(ref, ref, semaphore, semaphore, at(cc=1 - c)).wait_recv()

    def departed(ref, semaphore):
        remote(ref, ref, semaphore, semaphore, at(cc=1 - c)).wait_send()

    phase("a_signal")
    barrier = pltpu.get_barrier_semaphore()
    for d in range(NEAR, 0, -1):
        signal(barrier, zz=lax.rem(z + d, Z))
        signal(barrier, zz=lax.rem(z + Z - d, Z))
    for d in far_y:
        for cc in range(C):
            signal(barrier, yy=lax.rem(y + d, Y), cc=cc)
    for d in (2, 3, 1):
        for cc in range(C):
            signal(barrier, xx=lax.rem(x + d, X), cc=cc)
    signal(barrier, cc=1 - c)

    phase("b_load")
    lp_copy = pltpu.make_async_copy(last_peak, lp, small_sem.at[0])
    lp_copy.start()

    order = [lax.rem(mine + d, X * C) for d in far_k + (0,)]
    loads = [
        pltpu.make_async_copy(
            grads.at[pl.ds(pl.multiple_of(k * PIECE, 32), PIECE)],
            g.at[pl.ds(pl.multiple_of(k * PIECE, 32), PIECE)],
            load_sem.at[i],
        )
        for i, k in enumerate(order)
    ]
    for copy in loads:
        copy.start()
    state_copies = [
        pltpu.make_async_copy(src, state.at[i], small_sem.at[1 + i])
        for i, src in enumerate((master, moment1, moment2))
    ]
    for copy in state_copies:
        copy.start()
    lp_copy.wait()

    phase("c_inverse")
    square = (WIDTH, WIDTH)
    row_at = lax.broadcasted_iota(jnp.int32, square, 0)
    lane_at = lax.broadcasted_iota(jnp.int32, square, 1)
    for r in range(LANE_ROWS):
        inverse = code_limit / jnp.maximum(lp[pl.ds(r, 1), :], peak_floor)
        spread = jnp.where(row_at == lane_at, jnp.broadcast_to(inverse, square), 0.0)
        column = jnp.sum(spread, axis=1, keepdims=True)
        inv[pl.ds(r * WIDTH, WIDTH), :] = jnp.broadcast_to(column, square)

    def scaled(at_row, count):
        rows = pl.ds(pl.multiple_of(at_row, 8), count)
        return jnp.clip(g[rows, :] * inv[rows, :], -code_limit, code_limit)

    def encode(i):
        loads[i].wait()
        k = order[i]
        xx, cc = k // 2, lax.rem(k, 2)
        for n in range(2):
            pair = [scaled((4 * k + 2 * n + m) * GROUP, FIRST) for m in range(2)]
            codes_a[k, pl.ds(2 * n * FIRST, 2 * FIRST), :] = jnp.concatenate(pair, axis=0).astype(jnp.bfloat16)
        for n in range(4):
            codes_b[xx, 4 * cc + n] = scaled((4 * k + n) * GROUP + FIRST, LAST).astype(jnp.bfloat16)

    phase("d_first")
    encode(0)

    phase("e_barrier")
    pl.semaphore_wait(barrier, 2 * NEAR + (Y - 1) * C + (X - 1) * C + 1)

    phase("f_send1")
    mine_y = 2 * y + c
    sent_1a, got_1a, sent_1b, got_1b, sent_pk1, got_pk1 = (new_sem() for _ in range(6))

    def start(src, dst, semaphores, where):
        remote(src, dst, *semaphores, where).start()

    for i, k in enumerate(order):
        if i:
            encode(i)
        xx, cc = k // 2, lax.rem(k, 2)
        if i < X * C - 1:
            start(codes_a.at[k], r1a.at[mine], (sent_1a, got_1a), at(xx=xx, cc=cc))
        reader = xx // 2
        for n in (2, 3, 1):
            yy = 4 * cc + lax.rem(inside + n, 4)
            start(codes_b.at[xx, yy], r1b.at[mine_y, lax.rem(xx, 2)], (sent_1b, got_1b), at(yy=yy, cc=reader))
        yy = 4 * cc + inside

        @pl.when((yy != y) | (reader != c))
        def _(xx=xx, yy=yy, reader=reader):
            start(codes_b.at[xx, yy], r1b.at[mine_y, lax.rem(xx, 2)], (sent_1b, got_1b), at(yy=yy, cc=reader))

    phase("g_zround")
    signal(up, zz=lax.rem(z + NEAR, Z))
    signal(down, zz=lax.rem(z + Z - NEAR, Z))

    phase("h_peaks")
    tall = (GROUP, WIDTH)
    tall_row = lax.broadcasted_iota(jnp.int32, tall, 0)
    tall_lane = lax.broadcasted_iota(jnp.int32, tall, 1)
    for k in range(X * C):
        for i in range(4):
            rows = pl.ds((4 * k + i) * GROUP, GROUP)
            top = jnp.max(jnp.abs(g[rows, :]), axis=1, keepdims=True)
            laid = jnp.where(tall_row == tall_lane, jnp.broadcast_to(top, tall), 0.0)
            pk1[k, i : i + 1, :] = jnp.max(laid, axis=0, keepdims=True)
    for k in order[:-1]:
        remote(pk1.at[k], rp1.at[mine], sent_pk1, got_pk1, at(xx=k // 2, cc=lax.rem(k, 2))).start()

    phase("j_scale")
    first_row = (((x * Y + y) * C + c) * Z + z) * OWNED
    flat = lax.broadcasted_iota(jnp.int32, (LANE_ROWS, WIDTH), 0) * WIDTH + lax.broadcasted_iota(
        jnp.int32, (LANE_ROWS, WIDTH), 1
    )
    own_row = lax.broadcasted_iota(jnp.int32, (OWNED, WIDTH), 0)
    all_scales = jnp.maximum(lp[...], peak_floor) / code_limit
    scale = jnp.zeros((OWNED, WIDTH), jnp.float32)
    for j in range(OWNED):
        one = jnp.sum(jnp.where(flat == first_row + j, all_scales, 0.0), axis=(0, 1), keepdims=True)
        scale = jnp.where(own_row == j, jnp.broadcast_to(one, scale.shape), scale)

    def either(condition, kind, ref, semaphore, fewer, more):
        @pl.when(condition)
        def _():
            kind(ref.at[pl.ds(0, fewer)], semaphore)

        @pl.when(jnp.logical_not(condition))
        def _():
            kind(ref.at[pl.ds(0, more)], semaphore)

    phase("k_wait1a")
    arrived(r1a.at[pl.ds(0, X * C - 1)], got_1a)

    phase("l_sum1a")
    block = 80
    for n in range(2):
        total = codes_a[mine, pl.ds(n * block, block), :].astype(jnp.float32)
        for d in range(1, X * C):
            k = lax.rem(mine + d, X * C)
            total = total + r1a[k, pl.ds(n * block, block), :].astype(jnp.float32)
        for m in range(2):
            s1a[2 * n + m] = total[m * FIRST : m * FIRST + SHARE, :]
            s1b[2 * n + m] = total[m * FIRST + SHARE : (m + 1) * FIRST, :]

    phase("m_send2a")
    sent_2a, got_2a, sent_2b, got_2b, sent_p2, got_p2 = (new_sem() for _ in range(6))
    for d in (2, 3, 1):
        i = lax.rem(inside + d, 4)
        start(s1a.at[i], r2a.at[y], (sent_2a, got_2a), at(yy=4 * c + i, cc=0))
        start(s1b.at[i], r2b.at[y], (sent_2b, got_2b), at(yy=4 * c + i, cc=1))

    @pl.when(local & first_core)
    def _():
        r2a[y] = s1a[inside]

    @pl.when(jnp.logical_not(local & first_core))
    def _():
        start(s1a.at[inside], r2a.at[y], (sent_2a, got_2a), at(yy=4 * c + inside, cc=0))

    @pl.when(local & last_core)
    def _():
        r2b[y] = s1b[inside]

    @pl.when(jnp.logical_not(local & last_core))
    def _():
        start(s1b.at[inside], r2b.at[y], (sent_2b, got_2b), at(yy=4 * c + inside, cc=1))

    def to_y(source, landing, semaphores):
        for d in (2, 3, 1):
            for cc in range(C):
                i = lax.rem(inside + d, 4)
                start(source.at[i], landing, semaphores, at(yy=4 * c + i, cc=cc))
        start(source.at[inside], landing, semaphores, at(yy=4 * c + inside, cc=1 - c))

        @pl.when(jnp.logical_not(local))
        def _():
            start(source.at[inside], landing, semaphores, at(yy=4 * c + inside, cc=c))

    phase("n_peak1")
    arrived(rp1.at[pl.ds(0, X * C - 1)], got_pk1)
    top = pk1[mine]
    for d in range(1, X * C):
        top = jnp.maximum(top, rp1[lax.rem(mine + d, X * C)])
    for i in range(4):
        p1[i] = top[i : i + 1, :]
    to_y(p1, rp2.at[y], (sent_p2, got_p2))

    @pl.when(local)
    def _():
        rp2[y] = p1[inside]

    phase("o_wait1b")
    arrived(r1b.at[pl.ds(0, Y * C - 1)], got_1b)
    phase("p_sum1b")
    for j in range(2):
        total = codes_b[2 * c + j, y].astype(jnp.float32)
        for d in range(1, Y * C):
            total = total + r1b[lax.rem(mine_y + d, Y * C), j].astype(jnp.float32)
        s1c[j] = total
    sent_2c, got_2c = new_sem(), new_sem()
    own_c = (xhalf == c) & last_core
    i = 1 - xin
    start(s1c.at[i], r2c.at[x], (sent_2c, got_2c), at(xx=2 * c + i, cc=1))

    @pl.when(own_c)
    def _():
        r2c[x] = s1c[xin]

    @pl.when(jnp.logical_not(own_c))
    def _():
        start(s1c.at[xin], r2c.at[x], (sent_2c, got_2c), at(xx=2 * c + xin, cc=1))

    phase("pa_zround")
    pl.semaphore_wait(up, 1)
    pl.semaphore_wait(down, 1)

    phase("pb_wait2")

    @pl.when(first_core)
    def _():
        either(local, arrived, r2a, got_2a, Y - 1, Y)
        total = r2a[0]
        for i in range(1, Y):
            total = total + r2a[i]
        t36[...] = total

    @pl.when(last_core)
    def _():
        either(local, arrived, r2b, got_2b, Y - 1, Y)
        total = r2b[0]
        for i in range(1, Y):
            total = total + r2b[i]
        t36[0:SPLIT, :] = total
        either(xhalf == c, arrived, r2c, got_2c, X - 1, X)
        total = r2c[0]
        for i in range(1, X):
            total = total + r2c[i]
        t36[SPLIT:SHARE, :] = total

    phase("pc_sum2")
    for i in range(Z):
        s2[i] = t36[i * OWNED : (i + 1) * OWNED, :]

    phase("q_send3")
    sent_3, got_3, sent_p3, got_p3 = (new_sem() for _ in range(4))
    for d in far_z:
        zz = lax.rem(z + d, Z)
        start(s2.at[zz], r3.at[z], (sent_3, got_3), at(zz=zz))

    phase("r_peak2")
    either(local, arrived, rp2, got_p2, Y - 1, Y)
    top = rp2[0]
    for i in range(1, Y):
        top = jnp.maximum(top, rp2[i])
    p3[...] = top
    for d in far_z:
        start(p3, rp3.at[z], (sent_p3, got_p3), at(zz=lax.rem(z + d, Z)))

    for copy in state_copies:
        copy.wait()
    phase("s_wait3")
    arrived(r3.at[pl.ds(0, Z - 1)], got_3)
    phase("t_adam")
    total = s2[z]
    for d in range(1, Z):
        total = total + r3[lax.rem(z + d, Z)]
    gradient = total * scale
    updated, first, second = adamw(gradient, state[0], state[1], state[2])
    w3[...] = updated.astype(jnp.bfloat16).astype(jnp.float32)

    phase("u_givez")
    sent_z, got_z = new_sem(), new_sem()
    for d in far_z:
        start(w3, gz.at[z], (sent_z, got_z), at(zz=lax.rem(z + d, Z)))
    gz[z] = w3[...]
    stepped[0] = updated
    stepped[1] = first
    stepped[2] = second

    phase("v_peak3")
    arrived(rp3.at[pl.ds(0, Z - 1)], got_p3)
    top = p3[...]
    for d in range(1, Z):
        top = jnp.maximum(top, rp3[lax.rem(z + d, Z)])
    rp4[y] = top
    sent_p4, got_p4 = new_sem(), new_sem()
    for d in far_y:
        start(rp4.at[y], rp4.at[y], (sent_p4, got_p4), at(yy=lax.rem(y + d, Y)))

    phase("w_waitgz")
    arrived(gz.at[pl.ds(0, Z - 1)], got_z)
    phase("x_asm36")
    for i in range(Z):
        a36[pl.ds(i * OWNED, OWNED), :] = gz[i]
    ay[...] = a36[...].astype(jnp.bfloat16)
    a4[...] = a36[0:SPLIT, :]

    phase("y_givey")
    sent_ya, got_ya, sent_yb, got_yb, sent_xb, got_xb = (new_sem() for _ in range(6))

    def rows_b(xx, yy):
        return wb.at[xx, yy, pl.ds(FIRST, LAST)]

    @pl.when(last_core)
    def _():
        b32[...] = a36[SPLIT:SHARE, :].astype(jnp.bfloat16)
        for d in far_y:
            start(a4, gyb.at[inside], (sent_yb, got_yb), at(yy=lax.rem(y + d, Y), cc=half))
        for d in (2, 3, 1):
            start(b32, rows_b(x, y), (sent_xb, got_xb), at(xx=lax.rem(x + d, X), cc=xhalf))

        @pl.when(xhalf == 0)
        def _():
            start(b32, rows_b(x, y), (sent_xb, got_xb), at(cc=0))

        @pl.when(xhalf == 1)
        def _():
            wb[x, y, pl.ds(FIRST, LAST), :] = b32[...]

        @pl.when(local)
        def _():
            gyb[inside] = a4[...]

        @pl.when(jnp.logical_not(local))
        def _():
            start(a4, gyb.at[inside], (sent_yb, got_yb), at(cc=0))

    @pl.when(first_core)
    def _():
        for d in far_y:
            start(ay, gya.at[inside], (sent_ya, got_ya), at(yy=lax.rem(y + d, Y), cc=half))

        @pl.when(local)
        def _():
            gya[inside] = ay[...]

        @pl.when(jnp.logical_not(local))
        def _():
            start(ay, gya.at[inside], (sent_ya, got_ya), at(cc=1))

    phase("z_peakx")
    arrived(rp4.at[pl.ds(0, Y - 1)], got_p4)
    for i in range(Y):
        pg[i : i + 1, :] = rp4[i]
    sent_p5, got_p5 = new_sem(), new_sem()
    for d in (2, 3, 1):
        start(pg, rp5.at[x], (sent_p5, got_p5), at(xx=lax.rem(x + d, X)))
    rp5[x] = pg[...]

    phase("za_waitxb")
    sent_x, sent_yc, sent_core, got_core = (new_sem() for _ in range(4))
    either(own_c, arrived, r1b.at[0], got_xb, 1, 2)

    def part_b(yy):
        return wb.at[pl.ds(2 * c, 2), yy, pl.ds(FIRST, LAST)]

    for d in far_y:
        start(part_b(y), part_b(y), (sent_yc, ryb.at[y]), at(yy=lax.rem(y + d, Y)))
    start(part_b(y), part_b(y), (sent_core, got_core), at(cc=1 - c))

    phase("zb_waitya")
    either(local & first_core, arrived, gya, got_ya, 3, 4)
    either(local & last_core, arrived, gyb, got_yb, 3, 4)
    phase("zc_asm160")
    for i in range(4):
        t160[i * FIRST : i * FIRST + SHARE, :] = gya[i].astype(jnp.float32)
        t160[i * FIRST + SHARE : (i + 1) * FIRST, :] = gyb[i]
    for i in range(4):
        wb[x, 4 * c + i, pl.ds(0, FIRST), :] = t160[i * FIRST : (i + 1) * FIRST, :].astype(jnp.bfloat16)

    phase("zd_givex")

    def part_a(xx):
        return wb.at[xx, pl.ds(4 * c, 4), pl.ds(0, FIRST)]

    for d in (2, 3, 1):
        start(part_a(x), part_a(x), (sent_x, rxa.at[x]), at(xx=lax.rem(x + d, X)))
    start(part_a(x), part_a(x), (sent_core, got_core), at(cc=1 - c))

    phase("zd_peaks")
    arrived(rp5.at[pl.ds(0, X - 1)], got_p5)
    lane_of = lax.broadcasted_iota(jnp.int32, (1, WIDTH), 1)
    for j in range(LANE_ROWS):
        line = jnp.zeros((1, WIDTH), jnp.float32)
        for n in range(X * Y):
            lo = GROUP * n - WIDTH * j
            if lo >= WIDTH or lo + GROUP <= 0:
                continue
            row = rp5[n // Y, n % Y : n % Y + 1, :]
            if lo % WIDTH:
                row = pltpu.roll(row, lo % WIDTH, 1)
            line = jnp.where((lane_of >= lo) & (lane_of < lo + GROUP), row, line)
        peak_lanes[j : j + 1, :] = line

    phase("ze_waitlast")

    def from_y(d):
        yy = lax.rem(y + d, Y)
        arrived(part_b(yy), ryb.at[yy])
        start(part_b(yy), part_b(yy), (sent_core, got_core), at(cc=1 - c))

    def from_x(d):
        xx = lax.rem(x + d, X)
        arrived(part_a(xx), rxa.at[xx])
        start(part_a(xx), part_a(xx), (sent_core, got_core), at(cc=1 - c))

    from_y(1)
    from_y(7)
    from_y(2)
    from_y(6)
    from_x(1)
    from_x(3)
    from_y(3)
    from_y(5)
    from_y(4)
    from_x(2)

    phase("zf_drain")
    departed(r1a.at[pl.ds(0, X * C - 1)], sent_1a)
    departed(r1b.at[pl.ds(0, Y * C - 1)], sent_1b)
    departed(rp1.at[pl.ds(0, X * C - 1)], sent_pk1)
    either(local & first_core, departed, r2a, sent_2a, 3, 4)
    either(local & last_core, departed, r2b, sent_2b, 3, 4)
    either(own_c, departed, r2c, sent_2c, 1, 2)
    either(local, departed, rp2, sent_p2, 7, 8)
    departed(r3.at[pl.ds(0, Z - 1)], sent_3)
    departed(rp3.at[pl.ds(0, Z - 1)], sent_p3)
    departed(gz.at[pl.ds(0, Z - 1)], sent_z)
    departed(rp4.at[pl.ds(0, Y - 1)], sent_p4)
    departed(rp5.at[pl.ds(0, X - 1)], sent_p5)

    @pl.when(first_core)
    def _():
        either(local, departed, gya, sent_ya, 7, 8)

    @pl.when(last_core)
    def _():
        either(local, departed, gyb, sent_yb, 7, 8)
        either(xhalf == 0, departed, codes_b.at[0], sent_xb, 4, 3)

    departed(r1b.at[pl.ds(0, Y - 1)], sent_yc)
    departed(r1a.at[pl.ds(0, X - 1)], sent_x)
    departed(wb.at[pl.ds(0, 2)], sent_core)
    arrived(wb.at[pl.ds(0, 2)], got_core)
    phase(None)


SEMS = 34


def store(stepped, wb, peak_lanes, out_master, out_first, out_second, weights, out_peak, sem):
    copies = [pltpu.make_async_copy(wb, weights, sem.at[0])]
    for i, dst in enumerate((out_master, out_first, out_second)):
        copies.append(pltpu.make_async_copy(stepped.at[i], dst, sem.at[1 + i]))
    copies.append(pltpu.make_async_copy(peak_lanes, out_peak, sem.at[4]))
    for copy in copies:
        copy.start()
    for copy in copies:
        copy.wait()


def body(grads, last_peak, master, moment1, moment2):
    f32, bf16 = jnp.float32, jnp.bfloat16
    vmem = lambda *shape, dtype=f32: pltpu.VMEM(shape, dtype)
    dma = lambda n: pltpu.SemaphoreType.DMA((n,))
    own = jax.ShapeDtypeStruct((OWNED, WIDTH), f32)
    whole = jax.ShapeDtypeStruct((X, Y, GROUP, WIDTH), bf16)
    lanes = jax.ShapeDtypeStruct((LANE_ROWS, WIDTH), f32)
    in_vmem = pl.BlockSpec(memory_space=pltpu.VMEM)
    anywhere = pl.BlockSpec(memory_space=pl.ANY)
    held = pl.pallas_call(
        kernel,
        out_shape=[jax.ShapeDtypeStruct((3, OWNED, WIDTH), f32), whole, lanes],
        in_specs=[pl.BlockSpec(memory_space=pltpu.HBM)] * 5,
        out_specs=[in_vmem] * 3,
        scratch_shapes=[
            vmem(ROWS, WIDTH),
            vmem(LANE_ROWS, WIDTH),
            vmem(ROWS, WIDTH),
            vmem(3, OWNED, WIDTH),
            vmem(X * C, 4 * FIRST, WIDTH, dtype=bf16),
            vmem(X, Y, LAST, WIDTH, dtype=bf16),
            vmem(X * C, 4 * FIRST, WIDTH, dtype=bf16),
            vmem(Y * C, 2, LAST, WIDTH, dtype=bf16),
            vmem(X * C, 4, WIDTH),
            vmem(X * C, 4, WIDTH),
            vmem(4, SHARE, WIDTH),
            vmem(4, SPLIT, WIDTH),
            vmem(2, LAST, WIDTH),
            vmem(4, 1, WIDTH),
            vmem(Y, SHARE, WIDTH),
            vmem(Y, SPLIT, WIDTH),
            vmem(X, LAST, WIDTH),
            vmem(Y, 1, WIDTH),
            vmem(SHARE, WIDTH),
            vmem(Z, OWNED, WIDTH),
            vmem(Z, OWNED, WIDTH),
            vmem(1, WIDTH),
            vmem(Z, 1, WIDTH),
            vmem(OWNED, WIDTH),
            vmem(Z, OWNED, WIDTH),
            vmem(SHARE, WIDTH),
            vmem(SHARE, WIDTH, dtype=bf16),
            vmem(SPLIT, WIDTH),
            vmem(LAST, WIDTH, dtype=bf16),
            vmem(8, SHARE, WIDTH, dtype=bf16),
            vmem(8, SPLIT, WIDTH),
            vmem(Y, 1, WIDTH),
            vmem(4 * FIRST, WIDTH),
            vmem(Y, WIDTH),
            vmem(X, Y, WIDTH),
            pltpu.SemaphoreType.REGULAR,
            pltpu.SemaphoreType.REGULAR,
            dma(X * C), dma(4), dma(SEMS), dma(X), dma(Y),
        ],
        compiler_params=pltpu.CompilerParams(
            collective_id=0, has_side_effects=True, vmem_limit_bytes=16 * 2**20
        ),
    )(*(
        pltpu.with_memory_space_constraint(a, pltpu.HBM)
        for a in (grads.reshape(ROWS, WIDTH), last_peak.reshape(LANE_ROWS, WIDTH), master, moment1, moment2)
    ))
    updated, first, second, weights, peak = pl.pallas_call(
        store,
        out_shape=[own, own, own, whole, lanes],
        in_specs=[in_vmem] * 3,
        out_specs=[anywhere] * 5,
        scratch_shapes=[dma(5)],
        compiler_params=pltpu.CompilerParams(vmem_limit_bytes=8 * 2**20),
    )(*held)
    return (updated, first, second, weights.reshape(ROWS, WIDTH), peak.reshape(ROWS))


def solution(mesh):
    torus = Mesh(mesh.devices.reshape(X, Y, C, Z), AXES)
    in_specs = (P(AXES, None, None), P(), P(AXES, None), P(AXES, None), P(AXES, None))
    out_specs = (P(AXES, None), P(AXES, None), P(AXES, None), P(), P())
    return jax.shard_map(body, mesh=torus, in_specs=in_specs, out_specs=out_specs, check_vma=False)
```
